32 devices in a mesh: spin: 1 (over z), depth: 4 (over y), row: 4 (over x), col: 2 (over core).
Axes of the slice: x: 4, y: 4, z: 1, core: 2. Of those that a mesh axis runs over, the one named last changes fastest.
The devices are a block of a 4x4x8 slice.
Arguments:
- hamiltonian: float32 [6, 2048, 2048], P('spin', 'row', 'col')
- spec_bounds: float32 [6, 2], P('spin')
- occ_count: int32 [6], P('spin')
Outputs:
- output 1: float32 [6, 2048, 2048], P('spin', 'row', 'col')
- output 2: float32 [6], P('spin')
All inputs are finite; a program needn't handle non-finite values.
Results may differ from the reference program's by a relative error of at most 0.001.
Values sent between devices are 32-bit elements.
A program may use at most 768 MiB of HBM per device.

```python
import jax
import jax.numpy as jnp
from jax import lax

ORDER = 2048
KPTS = 6
STEPS = 3


def setup_inputs(seed: int = 0, part: int = 0) -> dict:
    key_base = jax.random.fold_in(jax.random.key(seed), part)
    key_off, key_site, key_shift, key_margin, key_occ = jax.random.split(key_base, 5)
    raw_off = jax.random.normal(key_off, (KPTS, ORDER, ORDER), jnp.float32)
    coup_scale = (0.5 / ORDER) ** 0.5
    coupling = (raw_off + jnp.swapaxes(raw_off, 1, 2)) * coup_scale
    site_draw = jax.random.uniform(key_site, (KPTS, ORDER), jnp.float32)
    site_shift = jax.random.uniform(key_shift, (KPTS, 1), jnp.float32, -1.5, -0.5)
    onsite = site_shift + 0.8 * site_draw * site_draw
    identity = jnp.eye(ORDER, dtype=jnp.float32)
    hamiltonian = coupling + onsite[:, :, None] * identity
    margin = jax.random.uniform(key_margin, (KPTS, 2), jnp.float32, 0.1, 1.5)
    lower_bd = jnp.min(onsite, axis=1) - 2.0 - margin[:, 0]
    upper_bd = jnp.max(onsite, axis=1) + 2.0 + margin[:, 1]
    spec_bounds = jnp.stack([lower_bd, upper_bd], axis=1)
    occ_count = jax.random.randint(key_occ, (KPTS,), ORDER * 3 // 20, ORDER * 3 // 8 + 1, dtype=jnp.int32)
    return {'hamiltonian': hamiltonian, 'spec_bounds': spec_bounds, 'occ_count': occ_count}


def purify_one(operands):
    hamilton, bounds_one, occ_one = operands
    highest = lax.Precision.HIGHEST
    occupied = occ_one.astype(jnp.float32)
    chem_pot = jnp.trace(hamilton) / ORDER
    scale_fac = jnp.minimum(occupied / (bounds_one[1] - chem_pot), (ORDER - occupied) / (chem_pot - bounds_one[0]))
    identity = jnp.eye(ORDER, dtype=jnp.float32)
    start_dens = (scale_fac / ORDER) * (chem_pot * identity - hamilton) + (occupied / ORDER) * identity

    def purify_step(density, unused):
        dens_sq = jnp.dot(density, density, precision=highest, preferred_element_type=jnp.float32)
        dens_cube = jnp.dot(dens_sq, density, precision=highest, preferred_element_type=jnp.float32)
        tr_one = jnp.trace(density)
        tr_two = jnp.sum(density * density)
        tr_three = jnp.sum(dens_sq * density)
        purify_coef = (tr_two - tr_three) / (tr_one - tr_two)
        new_dens = ((1.0 - 2.0 * purify_coef) * density + (1.0 + purify_coef) * dens_sq - dens_cube) / (1.0 - purify_coef)
        return new_dens, None

    final_dens, unused_out = lax.scan(purify_step, start_dens, None, length=STEPS)
    energy = 2.0 * jnp.sum(final_dens * hamilton)
    return final_dens, energy


def reference(hamiltonian, spec_bounds, occ_count):
    density, energy = lax.map(purify_one, (hamiltonian, spec_bounds, occ_count))
    return density, energy
```

```python
import functools

import jax
import jax.numpy as jnp
from jax import lax
from jax.experimental import pallas as pl
from jax.experimental.pallas import tpu as pltpu
from jax.sharding import PartitionSpec as P

STEPS = 3
MESH = pl.DeviceIdType.MESH
F32 = jnp.float32
HIGHEST = lax.Precision.HIGHEST


def dot_nn(a, b):
    return jnp.dot(a, b, precision=HIGHEST, preferred_element_type=F32)


def dot_nt(a, b):
    return lax.dot_general(a, b, (((1,), (1,)), ((), ())), precision=HIGHEST, preferred_element_type=F32)


def kernel(
    sizes, ham, bounds, occ, out, energy_out, relay,
    hb, xb, ps, pr, d3, ts, tr, es, er,
    in_send, in_recv_d, in_recv_o, tmp_send, tmp_recv,
    p_send, p_recv, t_send, t_recv,
    x_send, x_recv, r_send, r_recv, f_send, y_send, y_recv, e_send, e_recv, ey_send, ey_recv,
):
    slots, depth_size, row_size, col_size = sizes
    half = ham.shape[1]
    order = hb.shape[1]
    quarter = half // 2
    full_order = order * col_size
    spin = lax.axis_index('spin')
    q = lax.axis_index('depth')
    r = lax.axis_index('row')
    c = lax.axis_index('col')
    par = lax.rem(q, 2)
    grp = r // 2
    q_up = lax.rem(q + 1, depth_size)
    q_dn = lax.rem(q + depth_size - 1, depth_size)

    def dev(qq, rr, cc):
        return (spin, qq, rr, cc)

    def rcopy(src, dst, ssem, rsem, target):
        return pltpu.make_async_remote_copy(
            src_ref=src, dst_ref=dst, send_sem=ssem, recv_sem=rsem, device_id=target, device_id_type=MESH
        )

    def wait_for(dst, sem):
        pltpu.make_async_copy(dst, dst, sem).wait()

    def aligned(start, size):
        return pl.ds(pl.multiple_of(start, size), size)

    barrier = pltpu.get_barrier_semaphore()
    for dr in range(row_size):
        for dc in range(col_size):
            if dr or dc:
                target = dev(q, lax.rem(r + dr, row_size), lax.rem(c + dc, col_size))
                pl.semaphore_signal(barrier, inc=1, device_id=target, device_id_type=MESH)
    for qq in (q_up, q_dn):
        pl.semaphore_signal(barrier, inc=1, device_id=dev(qq, r, c), device_id_type=MESH)
    pl.semaphore_wait(barrier, row_size * col_size + 1)

    def in_parts(s):
        g = s // 2
        mat = par * slots + s
        full_half = ham.at[mat]
        diag_cols = aligned(lax.rem(r, 2) * half, half)
        rows = aligned(lax.rem(r, 2) * half, half)
        in_g = grp == g
        d_sender = c == grp
        own_d = jnp.logical_and(d_sender, r == s)
        far_full = jnp.logical_and(d_sender, jnp.logical_and(jnp.logical_not(in_g), lax.rem(r, 2) == 1 - s % 2))
        near_diag = jnp.logical_and(in_g, r != s)
        far_diag = jnp.logical_and(jnp.logical_not(in_g), lax.rem(r, 2) == s % 2)
        diag_only = jnp.logical_and(d_sender, jnp.logical_or(near_diag, far_diag))
        o_sender = jnp.logical_and(in_g, c != grp)
        dsem = in_recv_d.at[lax.rem(r, 2)]
        local = pltpu.make_async_copy(full_half, hb.at[0, rows], dsem)
        d_copy = rcopy(full_half, hb.at[0, rows], in_send.at[s], dsem, dev(q, s, grp))
        diag_copy = rcopy(ham.at[mat, :, diag_cols], hb.at[0, rows, diag_cols], in_send.at[s], dsem, dev(q, s, grp))
        o_copy = rcopy(full_half, hb.at[1, rows], in_send.at[s], in_recv_o.at[lax.rem(r, 2)], dev(q, s, g))
        return (own_d, local), ((far_full, d_copy), (diag_only, diag_copy), (o_sender, o_copy))

    for s in range(slots):
        (own_d, local), copies = in_parts(s)
        pl.when(own_d)(local.start)
        for cond, copy in copies:
            pl.when(cond)(copy.start)

    owner = r < slots
    alpha = c == grp
    mine = par * slots + jnp.minimum(r, slots - 1)
    peer = dev(q, r, 1 - c)

    def stat_exchange(k):
        return rcopy(ts.at[k], tr.at[k], t_send.at[k], t_recv.at[k], peer)

    def rowsum(x):
        return jnp.sum(x.reshape(x.shape[0] // 8, 8, x.shape[1]), axis=0)

    chunk = 128

    def chunks(body, init=None):
        return lax.fori_loop(0, order // chunk, lambda i, carry: body(aligned(i * chunk, chunk), i, carry), init)

    def total(v):
        return jnp.sum(jnp.sum(v, axis=1, keepdims=True), axis=0, keepdims=True)

    def tile(i):
        return aligned(i * half, half)

    def mirror(ref):
        ref[half:order, 0:half] = ref[0:half, half:order].T

    def eye_of(i):
        ids = lax.broadcasted_iota(jnp.int32, (chunk, order), 0) + i * chunk
        return ids == lax.broadcasted_iota(jnp.int32, (chunk, order), 1)

    def p_copy(slot, t):
        i, j = t // 2, lax.rem(t, 2)
        return rcopy(ps.at[tile(i), tile(j)], pr.at[slot, tile(i), tile(j)], p_send.at[t], p_recv.at[slot, t], peer)

    def send_product(slot, first, lhs, rhs):
        def body(t, _):
            i, j = t // 2, lax.rem(t, 2)
            if not first:
                p_copy(1 - slot, t).wait_send()
            ps[tile(i), tile(j)] = dot_nn(xb[lhs, tile(i), :], xb[rhs, :, tile(j)])
            p_copy(slot, t).start()
            return 0
        lax.fori_loop(0, 4, body, 0)

    def sym_product(dst, left):
        def body(t, _):
            i, j = t // 2, (t + 1) // 2
            dst[tile(i), tile(j)] = (
                dot_nn(xb[left, tile(i), :], xb[0, :, tile(j)]) + dot_nt(xb[left + 1, tile(i), :], xb[1, tile(j), :])
            )
            return 0
        lax.fori_loop(0, 3, body, 0)

    def summed(slot, i, j):
        return ps[tile(i), tile(j)] + pr[slot, tile(j), tile(i)].T

    @pl.when(owner)
    def _():
        own_half = lax.rem(r, 2)
        whole = jnp.where(alpha, own_half, 1 - own_half)
        other = 1 - whole
        rows_w = aligned(whole * half, half)
        rows_o = aligned(other * half, half)

        def tmp_copy(k):
            rows = pl.ds(k * half, half)
            return rcopy(hb.at[1, rows], pr.at[1, rows], tmp_send.at[k], tmp_recv.at[k], peer)

        @pl.when(alpha)
        def _():
            for k in range(2):
                wait_for(hb.at[1, pl.ds(k * half, half)], in_recv_o.at[k])
                tmp_copy(k).start()

        wait_for(hb.at[0, rows_o, rows_o], in_recv_d.at[other])
        wait_for(hb.at[0, rows_w], in_recv_d.at[whole])
        hb[0, rows_o, rows_w] = hb[0, rows_w, rows_o].T

        def trace_h(rows, i, acc):
            return acc + rowsum(jnp.where(eye_of(i), hb[0, rows, :], 0.0))
        ts[0, 0] = chunks(trace_h, jnp.zeros((8, order), F32))
        stat_exchange(0).start()

        @pl.when(jnp.logical_not(alpha))
        def _():
            for k in range(2):
                tmp_copy(k).wait_recv()
                hb[1, :, k * half:(k + 1) * half] = pr[1, k * half:(k + 1) * half, :].T

        @pl.when(alpha)
        def _():
            for k in range(2):
                tmp_copy(k).wait_send()

        stat_exchange(0).wait()
        n = float(full_order)
        mu = total(ts[0, 0] + tr[0, 0]) / n
        occupied = jnp.full((1, 1), occ[mine].astype(F32))
        eps_min = jnp.full((1, 1), bounds[mine, 0])
        eps_max = jnp.full((1, 1), bounds[mine, 1])
        lam = jnp.minimum(occupied / (eps_max - mu), (n - occupied) / (mu - eps_min))
        shift = (lam * mu + occupied) / n
        slope = lam / n

        def start_x(rows, i, _):
            xb[0, rows, :] = jnp.where(eye_of(i), shift, 0.0) - slope * hb[0, rows, :]
            xb[1, rows, :] = -(slope * hb[1, rows, :])
            return 0
        chunks(start_x, 0)

        for step in range(STEPS):
            send_product(0, step == 0, 0, 1)
            sym_product(xb.at[2], 0)
            mirror(xb.at[2])
            for t in range(4):
                i, j = t // 2, t % 2
                p_copy(0, j * 2 + i).wait_recv()
                xb[3, i * half:(i + 1) * half, j * half:(j + 1) * half] = summed(0, i, j)

            def stats(rows, i, acc):
                a1, a2, a3 = acc
                d, o = xb[0, rows, :], xb[1, rows, :]
                return (
                    a1 + rowsum(jnp.where(eye_of(i), d, 0.0)),
                    a2 + rowsum(d * d + o * o),
                    a3 + rowsum(xb[2, rows, :] * d + xb[3, rows, :] * o),
                )
            zero = jnp.zeros((8, order), F32)
            sums = chunks(stats, (zero, zero, zero))
            for k in range(3):
                ts[1 + step, k] = sums[k]
            stat_exchange(1 + step).start()

            send_product(1, False, jnp.where(alpha, 2, 0), jnp.where(alpha, 1, 3))
            sym_product(d3, 2)
            mirror(d3)
            stat_exchange(1 + step).wait()
            t1, t2, t3 = (total(ts[1 + step, k] + tr[1 + step, k]) for k in range(3))
            coef = (t2 - t3) / (t1 - t2)
            den = 1.0 - coef
            ca, cb = 1.0 - 2.0 * coef, 1.0 + coef

            def new_d(rows, i, _):
                xb[0, rows, :] = (ca * xb[0, rows, :] + cb * xb[2, rows, :] - d3[rows, :]) / den
                return 0
            chunks(new_d, 0)
            for t in range(4):
                i, j = t // 2, t % 2
                at = (slice(i * half, (i + 1) * half), slice(j * half, (j + 1) * half))
                p_copy(1, j * 2 + i).wait_recv()
                xb[1, at[0], at[1]] = (ca * xb[1, at[0], at[1]] + cb * xb[3, at[0], at[1]] - summed(1, i, j)) / den
        for t in range(4):
            p_copy(1, t).wait_send()

    def rows_of(h):
        return pl.ds(h * quarter, quarter)

    def x_copy(s, h, dr, target_core, hops):
        rr = (s + dr) % row_size
        core = rr // 2
        part = xb.at[jnp.where(core == target_core, 0, 1), pl.ds((rr % 2) * half + h * quarter, quarter)]
        mat = par * slots + s
        sem = x_send.at[dr, target_core, h]
        if hops == 0:
            return pltpu.make_async_copy(part, out.at[mat, rows_of(h)], x_recv.at[s, h])
        if hops == 1:
            return rcopy(part, out.at[mat, rows_of(h)], sem, x_recv.at[s, h], dev(q, rr, target_core))
        via = (s + 1) % row_size if h == 0 else (s + row_size - 1) % row_size
        return rcopy(part, relay.at[h], sem, r_recv.at[h], dev(q, via, target_core))

    def owner_copies(s):
        g = s // 2
        found = []
        for dr in (2, 1, 3, 0):
            rr = (s + dr) % row_size
            for target_core in range(col_size):
                for h in range(2):
                    here = dr == 0 and target_core == rr // 2
                    hops = 0 if here else 2 if dr == 2 else 1
                    found.append((rr // 2, hops, functools.partial(x_copy, s, h, dr, target_core, hops)))
        return g, found

    for s in range(slots):
        @pl.when(r == s)
        def _(s=s):
            for core, hops, make in owner_copies(s)[1]:
                pl.when(c == core)(lambda make=make: make().start())

    @pl.when(owner)
    def _():
        def energy_part(rows, i, acc):
            return acc + rowsum(xb[0, rows, :] * hb[0, rows, :] + xb[1, rows, :] * hb[1, rows, :])
        ts[STEPS + 1, 0] = chunks(energy_part, jnp.zeros((8, order), F32))
        stat_exchange(STEPS + 1).start()
        stat_exchange(STEPS + 1).wait()
        es[...] = jnp.broadcast_to(2.0 * total(ts[STEPS + 1, 0] + tr[STEPS + 1, 0]), es.shape)

    def e_copy(dr):
        return rcopy(es, er.at[mine], e_send.at[dr], e_recv.at[jnp.minimum(r, slots - 1)],
                     dev(q, lax.rem(r + dr, row_size), c))

    @pl.when(owner)
    def _():
        er[mine] = es[...]
        for dr in range(1, row_size):
            e_copy(dr).start()

    r_up = lax.rem(r + 1, row_size)
    r_dn = lax.rem(r + row_size - 1, row_size)
    for h in range(2):
        source = r_dn if h == 0 else r_up
        target = r_up if h == 0 else r_dn
        smat = par * slots + jnp.minimum(source, slots - 1)

        def relay_copy(h=h, source=source, target=target, smat=smat):
            return rcopy(relay.at[h], out.at[smat, rows_of(h)], r_send.at[h],
                         x_recv.at[jnp.minimum(source, slots - 1), h], dev(q, target, c))

        @pl.when(source < slots)
        def _(h=h, relay_copy=relay_copy):
            wait_for(relay.at[h], r_recv.at[h])
            relay_copy().start()

    def y_copy(s, h):
        part = out.at[par * slots + s, rows_of(h)]
        return rcopy(part, part, y_send.at[s, h], y_recv.at[s, h], dev(q_up if h == 0 else q_dn, r, c))

    def ey_copy(s):
        tile_ref = er.at[par * slots + s]
        return rcopy(tile_ref, tile_ref, ey_send.at[s], ey_recv.at[s], dev(q_up, r, c))

    for s in range(slots):
        for h in range(2):
            wait_for(out.at[par * slots + s, rows_of(h)], x_recv.at[s, h])
            y_copy(s, h).start()
    for s in range(slots):
        @pl.when(r != s)
        def _(s=s):
            wait_for(er.at[par * slots + s], e_recv.at[s])
        ey_copy(s).start()

    for s in range(slots):
        for h in range(2):
            wait_for(out.at[(1 - par) * slots + s, rows_of(h)], y_recv.at[s, h])
            y_copy(s, h).wait_send()
        wait_for(er.at[(1 - par) * slots + s], ey_recv.at[s])
        ey_copy(s).wait_send()

    for h in range(2):
        source = r_dn if h == 0 else r_up

        @pl.when(source < slots)
        def _(h=h):
            wait_for(relay.at[h], r_send.at[h])
    for s in range(slots):
        for cond, copy in in_parts(s)[1]:
            pl.when(cond)(copy.wait_send)

        @pl.when(r == s)
        def _(s=s):
            for core, hops, make in owner_copies(s)[1]:
                if hops:
                    pl.when(c == core)(lambda make=make: make().wait_send())

    @pl.when(owner)
    def _():
        for dr in range(1, row_size):
            e_copy(dr).wait_send()

    energy_out[...] = er[...]


def solution(mesh):
    depth_size = mesh.shape['depth']
    row_size = mesh.shape['row']
    col_size = mesh.shape['col']

    def local_purify(ham_blk, spec_bounds, occ_count):
        kpoints, row_blk, col_blk = ham_blk.shape
        slots = kpoints // 2
        any_space = pl.BlockSpec(memory_space=pl.ANY)
        smem = pl.BlockSpec(memory_space=pltpu.SMEM)
        vmem = pl.BlockSpec(memory_space=pltpu.VMEM)
        dma = pltpu.SemaphoreType.DMA
        square = (col_blk, col_blk)
        density, energy, _ = pl.pallas_call(
            functools.partial(kernel, (slots, depth_size, row_size, col_size)),
            out_shape=(
                jax.ShapeDtypeStruct(ham_blk.shape, F32),
                jax.ShapeDtypeStruct((kpoints, 8, 128), F32),
                jax.ShapeDtypeStruct((2, row_blk // 2, col_blk), F32),
            ),
            in_specs=[any_space, smem, smem],
            out_specs=(any_space, vmem, any_space),
            scratch_shapes=[
                pltpu.VMEM((2, *square), F32),
                pltpu.VMEM((4, *square), F32),
                pltpu.VMEM(square, F32),
                pltpu.VMEM((2, *square), F32),
                pltpu.VMEM(square, F32),
                pltpu.VMEM((STEPS + 2, 3, 8, col_blk), F32),
                pltpu.VMEM((STEPS + 2, 3, 8, col_blk), F32),
                pltpu.VMEM((8, 128), F32),
                pltpu.VMEM((kpoints, 8, 128), F32),
                dma((slots,)), dma((2,)), dma((2,)), dma((2,)), dma((2,)),
                dma((4,)), dma((2, 4)), dma((STEPS + 2,)), dma((STEPS + 2,)),
                dma((row_size, col_size, 2)), dma((slots, 2)), dma((2,)), dma((2,)), dma((2,)),
                dma((slots, 2)), dma((slots, 2)), dma((row_size,)), dma((slots,)), dma((slots,)), dma((slots,)),
            ],
            compiler_params=pltpu.CompilerParams(
                collective_id=0, has_side_effects=True, vmem_limit_bytes=60 * 2**20
            ),
            name='purify',
        )(ham_blk, spec_bounds, occ_count)
        return density, energy[:, 0, 0]

    mat_spec = P('spin', 'row', 'col')
    return jax.shard_map(local_purify, mesh=mesh, in_specs=(mat_spec, P('spin', None), P('spin')), out_specs=(mat_spec, P('spin')), check_vma=False)
```

```python
import functools

import jax
import jax.numpy as jnp
from jax import lax
from jax.experimental import pallas as pl
from jax.experimental.pallas import tpu as pltpu
from jax.sharding import PartitionSpec as P

STEPS = 3
PIECES = 4
MESH = pl.DeviceIdType.MESH
F32 = jnp.float32
HIGHEST = lax.Precision.HIGHEST


def dot_nn(a, b):
    return jnp.dot(a, b, precision=HIGHEST, preferred_element_type=F32)


def dot_nt(a, b):
    return lax.dot_general(a, b, (((1,), (1,)), ((), ())), precision=HIGHEST, preferred_element_type=F32)


def kernel(
    sizes, ham, bounds, occ, out, energy_out, relay,
    hb, xb, ps, pr, ts, tr, es, er,
    in_send, in_recv_d, in_recv_o, tmp_send, tmp_recv,
    p_send, p_recv, t_send, t_recv,
    x_send, x_recv, r_send, r_recv, y_send, y_recv, e_send, e_recv, ey_send, ey_recv,
):
    slots, depth_size, row_size, col_size = sizes
    half = ham.shape[1]
    order = hb.shape[1]
    piece = half // PIECES
    up_pieces = tuple(range(PIECES // 2))
    down_pieces = tuple(range(PIECES // 2, PIECES))
    in_turn = tuple(k for pair in zip(up_pieces, down_pieces) for k in pair)
    full_order = order * col_size
    spin = lax.axis_index('spin')
    q = lax.axis_index('depth')
    r = lax.axis_index('row')
    c = lax.axis_index('col')
    par = lax.rem(q, 2)
    grp = r // 2
    q_up = lax.rem(q + 1, depth_size)
    q_dn = lax.rem(q + depth_size - 1, depth_size)

    def dev(qq, rr, cc):
        return (spin, qq, rr, cc)

    def rcopy(src, dst, ssem, rsem, target):
        return pltpu.make_async_remote_copy(
            src_ref=src, dst_ref=dst, send_sem=ssem, recv_sem=rsem, device_id=target, device_id_type=MESH
        )

    def wait_for(dst, sem):
        pltpu.make_async_copy(dst, dst, sem).wait()

    def aligned(start, size):
        return pl.ds(pl.multiple_of(start, size), size)

    barrier = pltpu.get_barrier_semaphore()
    for dr in range(row_size):
        for dc in range(col_size):
            if dr or dc:
                target = dev(q, lax.rem(r + dr, row_size), lax.rem(c + dc, col_size))
                pl.semaphore_signal(barrier, inc=1, device_id=target, device_id_type=MESH)
    for qq in (q_up, q_dn):
        pl.semaphore_signal(barrier, inc=1, device_id=dev(qq, r, c), device_id_type=MESH)
    pl.semaphore_wait(barrier, row_size * col_size + 1)

    def slot_of(x):
        return jnp.where(x < slots, x, x - 2)

    def alone(x):
        return lax.rem(x, 2) == 0

    def in_parts(s):
        g = s // 2
        mat = par * slots + slot_of(s)
        full_half = ham.at[mat]
        diag_cols = aligned(lax.rem(r, 2) * half, half)
        rows = aligned(lax.rem(r, 2) * half, half)
        in_g = grp == g
        d_sender = c == grp
        own_d = jnp.logical_and(d_sender, r == s)
        far_full = jnp.logical_and(d_sender, jnp.logical_and(jnp.logical_not(in_g), lax.rem(r, 2) == 1 - s % 2))
        near_diag = jnp.logical_and(in_g, r != s)
        far_diag = jnp.logical_and(jnp.logical_not(in_g), lax.rem(r, 2) == s % 2)
        diag_only = jnp.logical_and(d_sender, jnp.logical_or(near_diag, far_diag))
        o_sender = jnp.logical_and(in_g, c != grp)
        dsem = in_recv_d.at[lax.rem(r, 2)]
        d_copy = rcopy(full_half, hb.at[0, rows], in_send.at[s], dsem, dev(q, s, grp))
        diag_copy = rcopy(ham.at[mat, :, diag_cols], hb.at[0, rows, diag_cols], in_send.at[s], dsem, dev(q, s, grp))
        o_copy = rcopy(full_half, hb.at[1, rows], in_send.at[s], in_recv_o.at[lax.rem(r, 2)], dev(q, s, g))
        def local():
            return pltpu.make_async_copy(full_half, hb.at[0, rows], dsem)
        return (own_d, local), ((far_full, d_copy), (diag_only, diag_copy), (o_sender, o_copy))

    for s in range(row_size):
        (own_d, local), copies = in_parts(s)
        pl.when(own_d)(lambda local=local: local().start())
        for cond, copy in copies:
            pl.when(cond)(copy.start)

    first_owner = r < slots
    my_slot = slot_of(r)
    alpha = c == grp
    mine = par * slots + my_slot
    peer = dev(q, r, 1 - c)
    final_d, final_o = (4, 5) if STEPS % 2 else (0, 1)

    def stat_exchange(k):
        return rcopy(ts.at[k], tr.at[k], t_send.at[k], t_recv.at[k], peer)

    def rowsum(x):
        return jnp.sum(x.reshape(x.shape[0] // 8, 8, x.shape[1]), axis=0)

    chunk = 128

    def chunks(body, init=None):
        return lax.fori_loop(0, order // chunk, lambda i, carry: body(aligned(i * chunk, chunk), i, carry), init)

    def total(v):
        return jnp.sum(jnp.sum(v, axis=1, keepdims=True), axis=0, keepdims=True)

    def tile(i):
        return aligned(i * half, half)

    def eye_of(i):
        ids = lax.broadcasted_iota(jnp.int32, (chunk, order), 0) + i * chunk
        return ids == lax.broadcasted_iota(jnp.int32, (chunk, order), 1)

    def diagonal(ref):
        ids = [lax.broadcasted_iota(jnp.int32, (chunk, chunk), k) for k in range(2)]
        acc = jnp.zeros((8, chunk), F32)
        for i in range(order // chunk):
            at = slice(i * chunk, (i + 1) * chunk)
            acc += rowsum(jnp.where(ids[0] == ids[1], ref[at, at], 0.0))
        return acc

    def rows_of(k):
        return pl.ds(k * piece, piece)

    def x_copy(which, dr, k):
        rr = lax.rem(r + dr, row_size)
        core = c if which == 0 else 1 - c
        start = lax.rem(rr, 2) * half + k * piece
        part = xb.at[final_o if which else final_d, aligned(start, piece)]
        sem = x_send.at[which, dr, k]
        arrived = x_recv.at[my_slot, k]
        if dr == 0 and which == 0:
            return pltpu.make_async_copy(part, out.at[mine, rows_of(k)], arrived)
        if dr != 2:
            return rcopy(part, out.at[mine, rows_of(k)], sem, arrived, dev(q, rr, core))
        via = lax.rem(r + (1 if k in up_pieces else row_size - 1), row_size)
        return rcopy(part, relay.at[k], sem, r_recv.at[k], dev(q, via, core))

    def sent_pieces(dr):
        shared = {0: in_turn, 1: up_pieces, 2: (), 3: down_pieces}[dr]
        return [(None if k in shared else alone(r), k) for k in in_turn]

    def guarded(cond, extra, action):
        pl.when(cond if extra is None else jnp.logical_and(cond, extra))(action)

    def x_starts(which, parity=None):
        for dr in (0, 2, 1, 3):
            rr = lax.rem(r + dr, row_size)
            cond = c == rr // 2
            if parity is not None:
                cond = jnp.logical_and(cond, lax.rem(rr, 2) == parity)
            for extra, k in sent_pieces(dr):
                guarded(cond, extra, lambda dr=dr, k=k: x_copy(which, dr, k).start())

    def p_copy(slot, t):
        i, j = t // 2, lax.rem(t, 2)
        return rcopy(ps.at[tile(i), tile(j)], pr.at[slot, tile(i), tile(j)], p_send.at[t], p_recv.at[slot, t], peer)

    def send_product(slot, lhs, rhs, before):
        def body(t, _):
            i, j = t // 2, lax.rem(t, 2)
            pl.when(before)(lambda: p_copy(1 - slot, t).wait_send())
            ps[tile(i), tile(j)] = dot_nn(xb[lhs, tile(i), :], xb[rhs, :, tile(j)])
            p_copy(slot, t).start()
            return 0
        lax.fori_loop(0, 4, body, 0)

    def purify():
        own_half = lax.rem(r, 2)
        whole = jnp.where(alpha, own_half, 1 - own_half)
        other = 1 - whole
        rows_w = aligned(whole * half, half)
        rows_o = aligned(other * half, half)

        def tmp_copy(k):
            rows = aligned(k * half, half)
            return rcopy(hb.at[1, rows], pr.at[1, rows], tmp_send.at[k], tmp_recv.at[k], peer)

        wait_for(hb.at[0, rows_o, rows_o], in_recv_d.at[other])
        wait_for(hb.at[0, rows_w], in_recv_d.at[whole])
        ts[0] = jnp.zeros(ts.shape[1:], F32)
        ts[0, 0, :, 0:chunk] = diagonal(hb.at[0])
        stat_exchange(0).start()
        hb[0, rows_o, rows_w] = hb[0, rows_w, rows_o].T

        @pl.when(alpha)
        def _():
            for k in (own_half, 1 - own_half):
                wait_for(hb.at[1, aligned(k * half, half)], in_recv_o.at[k])
                tmp_copy(k).start()

        @pl.when(jnp.logical_not(alpha))
        def _():
            for k in (own_half, 1 - own_half):
                tmp_copy(k).wait_recv()
                hb[1, :, aligned(k * half, half)] = pr[1, aligned(k * half, half), :].T

        @pl.when(alpha)
        def _():
            for k in range(2):
                tmp_copy(k).wait_send()

        stat_exchange(0).wait()
        n = float(full_order)
        mu = total(ts[0, 0] + tr[0, 0]) / n
        occupied = jnp.full((1, 1), occ[mine].astype(F32))
        eps_min = jnp.full((1, 1), bounds[0, mine])
        eps_max = jnp.full((1, 1), bounds[1, mine])
        lam = jnp.minimum(occupied / (eps_max - mu), (n - occupied) / (mu - eps_min))
        shift = (lam * mu + occupied) / n
        slope = lam / n

        def start_x(rows, i, _):
            xb[0, rows, :] = jnp.where(eye_of(i), shift, 0.0) - slope * hb[0, rows, :]
            xb[1, rows, :] = -(slope * hb[1, rows, :])
            return 0
        chunks(start_x, 0)

        def one_step(step, _):
            flip = lax.rem(step, 2)
            d_old, o_old = 4 * flip, 4 * flip + 1
            d_new, o_new = 4 - d_old, 6 - o_old
            k = 1 + step
            last = step == STEPS - 1

            ts[k] = jnp.zeros(ts.shape[1:], F32)
            ts[k, 0, :, 0:chunk] = diagonal(xb.at[d_old])
            send_product(0, d_old, o_old, step > 0)

            def join_sq(t):
                i, j = t // 2, lax.rem(t, 2)
                val = ps[tile(i), tile(j)] + pr[0, tile(j), tile(i)].T
                xb[3, tile(i), tile(j)] = val
                o = xb[o_old, tile(i), tile(j)]
                ts[k, 1] += rowsum(o * o)
                ts[k, 2] += rowsum(val * o)

            def sq_body(t, _):
                p_copy(0, lax.rem(t, 2) * 2 + t // 2).wait_recv()
                rows, cols = tile(t // 2), tile((t + 1) // 2)
                val = dot_nn(xb[d_old, rows, :], xb[d_old, :, cols]) + dot_nt(xb[o_old, rows, :], xb[o_old, cols, :])
                xb[2, rows, cols] = val
                d = xb[d_old, rows, cols]
                weight = jnp.where(t == 1, 2.0, 1.0)
                ts[k, 1] += weight * rowsum(d * d)
                ts[k, 2] += weight * rowsum(val * d)
                join_sq(t)

                @pl.when(t == 1)
                def _():
                    xb[2, half:order, 0:half] = xb[2, 0:half, half:order].T
                return 0
            lax.fori_loop(0, 3, sq_body, 0)
            p_copy(0, 3).wait_recv()
            join_sq(3)
            stat_exchange(k).start()

            send_product(1, jnp.where(c == 0, 2, d_old), jnp.where(c == 0, o_old, 3), True)
            stat_exchange(k).wait()
            t1, t2, t3 = (total(ts[k, i] + tr[k, i]) for i in range(3))
            coef = (t2 - t3) / (t1 - t2)
            inv = 1.0 / (1.0 - coef)
            ca, cb = (1.0 - 2.0 * coef) * inv, (1.0 + coef) * inv

            def join_new(t, _):
                i, j = t // 2, lax.rem(t, 2)
                p_copy(1, j * 2 + i).wait_recv()
                val = ps[tile(i), tile(j)] + pr[1, tile(j), tile(i)].T
                xb[o_new, tile(i), tile(j)] = ca * xb[o_old, tile(i), tile(j)] + cb * xb[3, tile(i), tile(j)] - inv * val
                return 0
            lax.fori_loop(0, 4, join_new, 0)
            pl.when(last)(lambda: x_starts(1))

            def cube_body(t, _):
                rows, cols = tile(t // 2), tile((t + 1) // 2)
                val = dot_nn(xb[2, rows, :], xb[d_old, :, cols]) + dot_nt(xb[3, rows, :], xb[o_old, cols, :])
                xb[d_new, rows, cols] = ca * xb[d_old, rows, cols] + cb * xb[2, rows, cols] - inv * val

                @pl.when(t == 1)
                def _():
                    xb[d_new, half:order, 0:half] = xb[d_new, 0:half, half:order].T
                for parity in range(2):
                    pl.when(jnp.logical_and(last, t == parity + 1))(lambda parity=parity: x_starts(0, parity))
                return 0
            lax.fori_loop(0, 3, cube_body, 0)
            return 0
        lax.fori_loop(0, STEPS, one_step, 0)
        for t in range(4):
            p_copy(1, t).wait_send()

    purify()

    def y_copy(s, k):
        part = out.at[par * slots + s, rows_of(k)]
        return rcopy(part, part, y_send.at[s, k], y_recv.at[s, k], dev(q_up if k in up_pieces else q_dn, r, c))

    def pass_on(cond, drs):
        for k in in_turn:
            for dr in drs:
                x = lax.rem(r + row_size - dr, row_size)
                shared = {0: in_turn, 1: up_pieces, 2: (), 3: down_pieces}[dr]

                def step_on(k=k, x=x):
                    at = slot_of(x)
                    wait_for(out.at[par * slots + at, rows_of(k)], x_recv.at[at, k])
                    y_copy(at, k).start()
                guarded(cond, None if k in shared else alone(x), step_on)

    r_up = lax.rem(r + 1, row_size)
    r_dn = lax.rem(r + row_size - 1, row_size)

    def relay_ends(k):
        return (r_dn, r_up) if k in up_pieces else (r_up, r_dn)

    def relay_copy(k):
        source, target = relay_ends(k)
        source = slot_of(source)
        return rcopy(relay.at[k], out.at[par * slots + source, rows_of(k)], r_send.at[k],
                     x_recv.at[source, k], dev(q, target, c))

    def relays(late):
        for k in in_turn:
            source, target = relay_ends(k)

            @pl.when(jnp.logical_and(alone(source), (c == target // 2) == late))
            def _(k=k):
                wait_for(relay.at[k], r_recv.at[k])
                relay_copy(k).start()

    early = c != grp
    pass_on(early, (0,))
    relays(False)
    pass_on(early, (1, 3))

    def e_copy(dr):
        return rcopy(es, er.at[mine], e_send.at[dr], e_recv.at[my_slot],
                     dev(q, lax.rem(r + dr, row_size), c))

    pass_on(jnp.logical_not(early), (0,))

    @pl.when(first_owner)
    def _():
        ts[STEPS + 1] = jnp.zeros(ts.shape[1:], F32)

        def energy_part(rows, i, _):
            v = rowsum(xb[final_d, rows, :] * hb[0, rows, :] + xb[final_o, rows, :] * hb[1, rows, :])
            ts[STEPS + 1, 0] += v[:, 0:half] + v[:, half:order]
            return 0
        chunks(energy_part, 0)
        stat_exchange(STEPS + 1).start()
        stat_exchange(STEPS + 1).wait()
        es[...] = jnp.broadcast_to(2.0 * total(ts[STEPS + 1, 0] + tr[STEPS + 1, 0]), es.shape)
        er[mine] = es[...]
        for dr in range(1, row_size):
            e_copy(dr).start()

    relays(True)
    pass_on(early, (2,))
    pass_on(jnp.logical_not(early), (1, 3))
    pass_on(jnp.logical_not(early), (2,))

    def ey_copy(s):
        tile_ref = er.at[par * slots + s]
        return rcopy(tile_ref, tile_ref, ey_send.at[s], ey_recv.at[s], dev(q_up, r, c))

    for s in range(slots):
        @pl.when(r != s)
        def _(s=s):
            wait_for(er.at[par * slots + s], e_recv.at[s])
        ey_copy(s).start()

    for s in range(slots):
        for k in range(PIECES):
            wait_for(out.at[(1 - par) * slots + s, rows_of(k)], y_recv.at[s, k])
            y_copy(s, k).wait_send()
        wait_for(er.at[(1 - par) * slots + s], ey_recv.at[s])
        ey_copy(s).wait_send()

    for k in range(PIECES):
        @pl.when(alone(relay_ends(k)[0]))
        def _(k=k):
            relay_copy(k).wait_send()
    for s in range(row_size):
        for cond, copy in in_parts(s)[1]:
            pl.when(cond)(copy.wait_send)

    for which in range(2):
        for dr in range(row_size):
            if which == 0 and dr == 0:
                continue
            for extra, k in sent_pieces(dr):
                guarded(c == lax.rem(r + dr, row_size) // 2, extra,
                        lambda which=which, dr=dr, k=k: x_copy(which, dr, k).wait_send())

    @pl.when(first_owner)
    def _():
        for dr in range(1, row_size):
            e_copy(dr).wait_send()

    energy_out[...] = er[...]


def solution(mesh):
    depth_size = mesh.shape['depth']
    row_size = mesh.shape['row']
    col_size = mesh.shape['col']

    def local_purify(ham_blk, spec_bounds, occ_count):
        kpoints, row_blk, col_blk = ham_blk.shape
        slots = kpoints // 2
        any_space = pl.BlockSpec(memory_space=pl.ANY)
        smem = pl.BlockSpec(memory_space=pltpu.SMEM)
        vmem = pl.BlockSpec(memory_space=pltpu.VMEM)
        dma = pltpu.SemaphoreType.DMA
        square = (col_blk, col_blk)
        density, energy, _ = pl.pallas_call(
            functools.partial(kernel, (slots, depth_size, row_size, col_size)),
            out_shape=(
                jax.ShapeDtypeStruct(ham_blk.shape, F32),
                jax.ShapeDtypeStruct((kpoints, 8, 128), F32),
                jax.ShapeDtypeStruct((PIECES, row_blk // PIECES, col_blk), F32),
            ),
            in_specs=[any_space, smem, smem],
            out_specs=(any_space, vmem, any_space),
            scratch_shapes=[
                pltpu.VMEM((2, *square), F32),
                pltpu.VMEM((6, *square), F32),
                pltpu.VMEM(square, F32),
                pltpu.VMEM((2, *square), F32),
                pltpu.VMEM((STEPS + 2, 3, 8, row_blk), F32),
                pltpu.VMEM((STEPS + 2, 3, 8, row_blk), F32),
                pltpu.VMEM((8, 128), F32),
                pltpu.VMEM((kpoints, 8, 128), F32),
                dma((row_size,)), dma((2,)), dma((2,)), dma((2,)), dma((2,)),
                dma((4,)), dma((2, 4)), dma((STEPS + 2,)), dma((STEPS + 2,)),
                dma((2, row_size, PIECES)), dma((slots, PIECES)), dma((PIECES,)), dma((PIECES,)),
                dma((slots, PIECES)), dma((slots, PIECES)), dma((row_size,)), dma((slots,)), dma((slots,)), dma((slots,)),
            ],
            compiler_params=pltpu.CompilerParams(
                collective_id=0, has_side_effects=True, vmem_limit_bytes=60 * 2**20
            ),
            name='purify',
        )(ham_blk, spec_bounds.T, occ_count)
        return density, energy[:, 0, 0]

    mat_spec = P('spin', 'row', 'col')
    return jax.shard_map(local_purify, mesh=mesh, in_specs=(mat_spec, P('spin', None), P('spin')), out_specs=(mat_spec, P('spin')), check_vma=False)
```

```python
import functools

import jax
import jax.numpy as jnp
from jax import lax
from jax.experimental import pallas as pl
from jax.experimental.pallas import tpu as pltpu
from jax.sharding import PartitionSpec as P

STEPS = 3
PIECES = 4
MESH = pl.DeviceIdType.MESH
F32 = jnp.float32
HIGHEST = lax.Precision.HIGHEST


def dot_nn(a, b):
    return jnp.dot(a, b, precision=HIGHEST, preferred_element_type=F32)


def dot_nt(a, b):
    return lax.dot_general(a, b, (((1,), (1,)), ((), ())), precision=HIGHEST, preferred_element_type=F32)


def kernel(
    sizes, ham, bounds, occ, out, energy_out, relay,
    hb, xb, ps, pr, ts, tr, es, er,
    in_send, in_recv_d, in_recv_o, tmp_send, tmp_recv,
    p_send, p_recv, t_send, t_recv,
    x_send, x_recv, r_send, r_recv, y_send, y_recv, e_send, e_recv, ey_send, ey_recv,
):
    slots, depth_size, row_size, col_size = sizes
    half = ham.shape[1]
    order = hb.shape[1]
    piece = half // PIECES
    up_pieces = tuple(range(PIECES // 2))
    down_pieces = tuple(range(PIECES // 2, PIECES))
    in_turn = tuple(k for pair in zip(up_pieces, down_pieces) for k in pair)
    full_order = order * col_size
    spin = lax.axis_index('spin')
    q = lax.axis_index('depth')
    r = lax.axis_index('row')
    c = lax.axis_index('col')
    par = lax.rem(q, 2)
    grp = r // 2
    q_up = lax.rem(q + 1, depth_size)
    q_dn = lax.rem(q + depth_size - 1, depth_size)

    def dev(qq, rr, cc):
        return (spin, qq, rr, cc)

    def rcopy(src, dst, ssem, rsem, target):
        return pltpu.make_async_remote_copy(
            src_ref=src, dst_ref=dst, send_sem=ssem, recv_sem=rsem, device_id=target, device_id_type=MESH
        )

    def wait_for(dst, sem):
        pltpu.make_async_copy(dst, dst, sem).wait()

    def aligned(start, size):
        return pl.ds(pl.multiple_of(start, size), size)

    barrier = pltpu.get_barrier_semaphore()
    for dr in range(row_size):
        for dc in range(col_size):
            if dr or dc:
                target = dev(q, lax.rem(r + dr, row_size), lax.rem(c + dc, col_size))
                pl.semaphore_signal(barrier, inc=1, device_id=target, device_id_type=MESH)
    for qq in (q_up, q_dn):
        pl.semaphore_signal(barrier, inc=1, device_id=dev(qq, r, c), device_id_type=MESH)
    pl.semaphore_wait(barrier, row_size * col_size + 1)

    def slot_of(x):
        return jnp.where(x < slots, x, x - 2)

    def alone(x):
        return lax.rem(x, 2) == 0

    def in_parts(s):
        g = s // 2
        mat = par * slots + slot_of(s)
        full_half = ham.at[mat]
        diag_cols = aligned(lax.rem(r, 2) * half, half)
        rows = aligned(lax.rem(r, 2) * half, half)
        in_g = grp == g
        d_sender = c == grp
        own_d = jnp.logical_and(d_sender, r == s)
        far_full = jnp.logical_and(d_sender, jnp.logical_and(jnp.logical_not(in_g), lax.rem(r, 2) == 1 - s % 2))
        near_diag = jnp.logical_and(in_g, r != s)
        far_diag = jnp.logical_and(jnp.logical_not(in_g), lax.rem(r, 2) == s % 2)
        diag_only = jnp.logical_and(d_sender, jnp.logical_or(near_diag, far_diag))
        o_sender = jnp.logical_and(in_g, c != grp)
        dsem = in_recv_d.at[lax.rem(r, 2)]
        d_copy = rcopy(full_half, hb.at[0, rows], in_send.at[s], dsem, dev(q, s, grp))
        diag_copy = rcopy(ham.at[mat, :, diag_cols], hb.at[0, rows, diag_cols], in_send.at[s], dsem, dev(q, s, grp))
        o_copy = rcopy(full_half, hb.at[1, rows], in_send.at[s], in_recv_o.at[lax.rem(r, 2)], dev(q, s, g))
        def local():
            return pltpu.make_async_copy(full_half, hb.at[0, rows], dsem)
        return (own_d, local), ((far_full, d_copy), (diag_only, diag_copy), (o_sender, o_copy))

    for s in range(row_size):
        (own_d, local), copies = in_parts(s)
        pl.when(own_d)(lambda local=local: local().start())
        for cond, copy in copies:
            pl.when(cond)(copy.start)

    first_owner = r < slots
    my_slot = slot_of(r)
    alpha = c == grp
    mine = par * slots + my_slot
    peer = dev(q, r, 1 - c)
    final_d, final_o = (4, 5) if STEPS % 2 else (0, 1)

    def stat_exchange(k):
        return rcopy(ts.at[k], tr.at[k], t_send.at[k], t_recv.at[k], peer)

    def rowsum(x):
        return jnp.sum(x.reshape(x.shape[0] // 8, 8, x.shape[1]), axis=0)

    chunk = 128

    def chunks(body, init=None):
        return lax.fori_loop(0, order // chunk, lambda i, carry: body(aligned(i * chunk, chunk), i, carry), init)

    def total(v):
        return jnp.sum(jnp.sum(v, axis=1, keepdims=True), axis=0, keepdims=True)

    def tile(i):
        return aligned(i * half, half)

    def eye_of(i):
        ids = lax.broadcasted_iota(jnp.int32, (chunk, order), 0) + i * chunk
        return ids == lax.broadcasted_iota(jnp.int32, (chunk, order), 1)

    def diagonal(ref):
        ids = [lax.broadcasted_iota(jnp.int32, (chunk, chunk), k) for k in range(2)]
        acc = jnp.zeros((8, chunk), F32)
        for i in range(order // chunk):
            at = slice(i * chunk, (i + 1) * chunk)
            acc += rowsum(jnp.where(ids[0] == ids[1], ref[at, at], 0.0))
        return acc

    def rows_of(k):
        return pl.ds(k * piece, piece)

    def x_copy(which, dr, k):
        rr = lax.rem(r + dr, row_size)
        core = c if which == 0 else 1 - c
        start = lax.rem(rr, 2) * half + k * piece
        part = xb.at[final_o if which else final_d, aligned(start, piece)]
        sem = x_send.at[which, dr, k]
        arrived = x_recv.at[my_slot, k]
        if dr == 0 and which == 0:
            return pltpu.make_async_copy(part, out.at[mine, rows_of(k)], arrived)
        if dr != 2:
            return rcopy(part, out.at[mine, rows_of(k)], sem, arrived, dev(q, rr, core))
        via = lax.rem(r + (1 if k in up_pieces else row_size - 1), row_size)
        return rcopy(part, relay.at[k], sem, r_recv.at[k], dev(q, via, core))

    def sent_pieces(dr):
        shared = {0: in_turn, 1: up_pieces, 2: (), 3: down_pieces}[dr]
        return [(None if k in shared else alone(r), k) for k in in_turn]

    def guarded(cond, extra, action):
        pl.when(cond if extra is None else jnp.logical_and(cond, extra))(action)

    def x_starts(which, parity=None):
        for dr in (0, 2, 1, 3):
            rr = lax.rem(r + dr, row_size)
            cond = c == rr // 2
            if parity is not None:
                cond = jnp.logical_and(cond, lax.rem(rr, 2) == parity)
            for extra, k in sent_pieces(dr):
                guarded(cond, extra, lambda dr=dr, k=k: x_copy(which, dr, k).start())

    def p_copy(slot, t):
        i, j = t // 2, lax.rem(t, 2)
        return rcopy(ps.at[tile(i), tile(j)], pr.at[slot, tile(i), tile(j)], p_send.at[t], p_recv.at[slot, t], peer)

    def send_product(slot, lhs, rhs, before):
        def body(t, _):
            i, j = t // 2, lax.rem(t, 2)
            pl.when(before)(lambda: p_copy(1 - slot, t).wait_send())
            ps[tile(i), tile(j)] = dot_nn(xb[lhs, tile(i), :], xb[rhs, :, tile(j)])
            p_copy(slot, t).start()
            return 0
        lax.fori_loop(0, 4, body, 0)

    def purify():
        own_half = lax.rem(r, 2)
        whole = jnp.where(alpha, own_half, 1 - own_half)
        other = 1 - whole
        rows_w = aligned(whole * half, half)
        rows_o = aligned(other * half, half)

        def tmp_copy(k):
            rows = aligned(k * half, half)
            return rcopy(hb.at[1, rows], pr.at[1, rows], tmp_send.at[k], tmp_recv.at[k], peer)

        wait_for(hb.at[0, rows_o, rows_o], in_recv_d.at[other])
        wait_for(hb.at[0, rows_w], in_recv_d.at[whole])
        ts[0] = jnp.zeros(ts.shape[1:], F32)
        ts[0, 0, :, 0:chunk] = diagonal(hb.at[0])
        stat_exchange(0).start()
        hb[0, rows_o, rows_w] = hb[0, rows_w, rows_o].T

        @pl.when(alpha)
        def _():
            for k in (own_half, 1 - own_half):
                wait_for(hb.at[1, aligned(k * half, half)], in_recv_o.at[k])
                tmp_copy(k).start()

        @pl.when(jnp.logical_not(alpha))
        def _():
            for k in (own_half, 1 - own_half):
                tmp_copy(k).wait_recv()
                hb[1, :, aligned(k * half, half)] = pr[1, aligned(k * half, half), :].T

        @pl.when(alpha)
        def _():
            for k in range(2):
                tmp_copy(k).wait_send()

        stat_exchange(0).wait()
        n = float(full_order)
        mu = total(ts[0, 0] + tr[0, 0]) / n
        occupied = jnp.full((1, 1), occ[mine].astype(F32))
        eps_min = jnp.full((1, 1), bounds[0, mine])
        eps_max = jnp.full((1, 1), bounds[1, mine])
        lam = jnp.minimum(occupied / (eps_max - mu), (n - occupied) / (mu - eps_min))
        shift = (lam * mu + occupied) / n
        slope = lam / n

        def start_x(rows, i, _):
            xb[0, rows, :] = jnp.where(eye_of(i), shift, 0.0) - slope * hb[0, rows, :]
            xb[1, rows, :] = -(slope * hb[1, rows, :])
            return 0
        chunks(start_x, 0)

        def one_step(step, _):
            flip = lax.rem(step, 2)
            d_old, o_old = 4 * flip, 4 * flip + 1
            d_new, o_new = 4 - d_old, 6 - o_old
            k = 1 + step
            last = step == STEPS - 1

            ts[k] = jnp.zeros(ts.shape[1:], F32)
            ts[k, 0, :, 0:chunk] = diagonal(xb.at[d_old])
            send_product(0, d_old, o_old, step > 0)

            def join_sq(t):
                i, j = t // 2, lax.rem(t, 2)
                val = ps[tile(i), tile(j)] + pr[0, tile(j), tile(i)].T
                xb[3, tile(i), tile(j)] = val
                o = xb[o_old, tile(i), tile(j)]
                ts[k, 1] += rowsum(o * o)
                ts[k, 2] += rowsum(val * o)

            def sq_body(t, _):
                p_copy(0, lax.rem(t, 2) * 2 + t // 2).wait_recv()
                rows, cols = tile(t // 2), tile((t + 1) // 2)
                val = dot_nn(xb[d_old, rows, :], xb[d_old, :, cols]) + dot_nt(xb[o_old, rows, :], xb[o_old, cols, :])
                xb[2, rows, cols] = val
                d = xb[d_old, rows, cols]
                weight = jnp.where(t == 1, 2.0, 1.0)
                ts[k, 1] += weight * rowsum(d * d)
                ts[k, 2] += weight * rowsum(val * d)
                join_sq(t)

                @pl.when(t == 1)
                def _():
                    xb[2, half:order, 0:half] = xb[2, 0:half, half:order].T
                return 0
            lax.fori_loop(0, 3, sq_body, 0)
            p_copy(0, 3).wait_recv()
            join_sq(3)
            stat_exchange(k).start()

            send_product(1, jnp.where(c == 0, 2, d_old), jnp.where(c == 0, o_old, 3), True)
            stat_exchange(k).wait()
            t1, t2, t3 = (total(ts[k, i] + tr[k, i]) for i in range(3))
            coef = (t2 - t3) / (t1 - t2)
            inv = 1.0 / (1.0 - coef)
            ca, cb = (1.0 - 2.0 * coef) * inv, (1.0 + coef) * inv

            def join_new(t, _):
                i, j = t // 2, lax.rem(t, 2)
                p_copy(1, j * 2 + i).wait_recv()
                val = ps[tile(i), tile(j)] + pr[1, tile(j), tile(i)].T
                xb[o_new, tile(i), tile(j)] = ca * xb[o_old, tile(i), tile(j)] + cb * xb[3, tile(i), tile(j)] - inv * val
                return 0
            lax.fori_loop(0, 4, join_new, 0)
            pl.when(last)(lambda: x_starts(1))

            def cube_body(t, _):
                rows, cols = tile(t // 2), tile((t + 1) // 2)
                val = dot_nn(xb[2, rows, :], xb[d_old, :, cols]) + dot_nt(xb[3, rows, :], xb[o_old, cols, :])
                xb[d_new, rows, cols] = ca * xb[d_old, rows, cols] + cb * xb[2, rows, cols] - inv * val

                @pl.when(t == 1)
                def _():
                    xb[d_new, half:order, 0:half] = xb[d_new, 0:half, half:order].T
                pl.when(jnp.logical_and(last, t == 0))(lambda: pass_on(early, (0,)))
                for parity in range(2):
                    pl.when(jnp.logical_and(last, t == parity + 1))(lambda parity=parity: x_starts(0, parity))
                return 0
            lax.fori_loop(0, 3, cube_body, 0)
            return 0
        lax.fori_loop(0, STEPS, one_step, 0)
        for t in range(4):
            p_copy(1, t).wait_send()

    def y_copy(s, k):
        part = out.at[par * slots + s, rows_of(k)]
        return rcopy(part, part, y_send.at[s, k], y_recv.at[s, k], dev(q_up if k in up_pieces else q_dn, r, c))

    def pass_on(cond, drs):
        for k in in_turn:
            for dr in drs:
                x = lax.rem(r + row_size - dr, row_size)
                shared = {0: in_turn, 1: up_pieces, 2: (), 3: down_pieces}[dr]

                def step_on(k=k, x=x):
                    at = slot_of(x)
                    wait_for(out.at[par * slots + at, rows_of(k)], x_recv.at[at, k])
                    y_copy(at, k).start()
                guarded(cond, None if k in shared else alone(x), step_on)

    r_up = lax.rem(r + 1, row_size)
    r_dn = lax.rem(r + row_size - 1, row_size)

    def relay_ends(k):
        return (r_dn, r_up) if k in up_pieces else (r_up, r_dn)

    def relay_copy(k):
        source, target = relay_ends(k)
        source = slot_of(source)
        return rcopy(relay.at[k], out.at[par * slots + source, rows_of(k)], r_send.at[k],
                     x_recv.at[source, k], dev(q, target, c))

    def relays(late):
        for k in in_turn:
            source, target = relay_ends(k)

            @pl.when(jnp.logical_and(alone(source), (c == target // 2) == late))
            def _(k=k):
                wait_for(relay.at[k], r_recv.at[k])
                relay_copy(k).start()

    early = c != grp
    purify()
    relays(False)
    pass_on(early, (1, 3))

    def e_copy(dr):
        return rcopy(es, er.at[mine], e_send.at[dr], e_recv.at[my_slot],
                     dev(q, lax.rem(r + dr, row_size), c))

    pass_on(jnp.logical_not(early), (0,))

    @pl.when(first_owner)
    def _():
        ts[STEPS + 1] = jnp.zeros(ts.shape[1:], F32)

        def energy_part(rows, i, _):
            v = rowsum(xb[final_d, rows, :] * hb[0, rows, :] + xb[final_o, rows, :] * hb[1, rows, :])
            ts[STEPS + 1, 0] += v[:, 0:half] + v[:, half:order]
            return 0
        chunks(energy_part, 0)
        stat_exchange(STEPS + 1).start()
        stat_exchange(STEPS + 1).wait()
        es[...] = jnp.broadcast_to(2.0 * total(ts[STEPS + 1, 0] + tr[STEPS + 1, 0]), es.shape)
        er[mine] = es[...]
        for dr in range(1, row_size):
            e_copy(dr).start()

    relays(True)
    pass_on(early, (2,))
    pass_on(jnp.logical_not(early), (1, 3))
    pass_on(jnp.logical_not(early), (2,))

    def ey_copy(s):
        tile_ref = er.at[par * slots + s]
        return rcopy(tile_ref, tile_ref, ey_send.at[s], ey_recv.at[s], dev(q_up, r, c))

    for s in range(slots):
        @pl.when(r != s)
        def _(s=s):
            wait_for(er.at[par * slots + s], e_recv.at[s])
        ey_copy(s).start()

    for s in range(slots):
        for k in range(PIECES):
            wait_for(out.at[(1 - par) * slots + s, rows_of(k)], y_recv.at[s, k])
            y_copy(s, k).wait_send()
        wait_for(er.at[(1 - par) * slots + s], ey_recv.at[s])
        ey_copy(s).wait_send()

    for k in range(PIECES):
        @pl.when(alone(relay_ends(k)[0]))
        def _(k=k):
            relay_copy(k).wait_send()
    for s in range(row_size):
        for cond, copy in in_parts(s)[1]:
            pl.when(cond)(copy.wait_send)

    for which in range(2):
        for dr in range(row_size):
            if which == 0 and dr == 0:
                continue
            for extra, k in sent_pieces(dr):
                guarded(c == lax.rem(r + dr, row_size) // 2, extra,
                        lambda which=which, dr=dr, k=k: x_copy(which, dr, k).wait_send())

    @pl.when(first_owner)
    def _():
        for dr in range(1, row_size):
            e_copy(dr).wait_send()

    energy_out[...] = er[...]


def solution(mesh):
    depth_size = mesh.shape['depth']
    row_size = mesh.shape['row']
    col_size = mesh.shape['col']

    def local_purify(ham_blk, spec_bounds, occ_count):
        kpoints, row_blk, col_blk = ham_blk.shape
        slots = kpoints // 2
        any_space = pl.BlockSpec(memory_space=pl.ANY)
        smem = pl.BlockSpec(memory_space=pltpu.SMEM)
        vmem = pl.BlockSpec(memory_space=pltpu.VMEM)
        dma = pltpu.SemaphoreType.DMA
        square = (col_blk, col_blk)
        density, energy, _ = pl.pallas_call(
            functools.partial(kernel, (slots, depth_size, row_size, col_size)),
            out_shape=(
                jax.ShapeDtypeStruct(ham_blk.shape, F32),
                jax.ShapeDtypeStruct((kpoints, 8, 128), F32),
                jax.ShapeDtypeStruct((PIECES, row_blk // PIECES, col_blk), F32),
            ),
            in_specs=[any_space, smem, smem],
            out_specs=(any_space, vmem, any_space),
            scratch_shapes=[
                pltpu.VMEM((2, *square), F32),
                pltpu.VMEM((6, *square), F32),
                pltpu.VMEM(square, F32),
                pltpu.VMEM((2, *square), F32),
                pltpu.VMEM((STEPS + 2, 3, 8, row_blk), F32),
                pltpu.VMEM((STEPS + 2, 3, 8, row_blk), F32),
                pltpu.VMEM((8, 128), F32),
                pltpu.VMEM((kpoints, 8, 128), F32),
                dma((row_size,)), dma((2,)), dma((2,)), dma((2,)), dma((2,)),
                dma((4,)), dma((2, 4)), dma((STEPS + 2,)), dma((STEPS + 2,)),
                dma((2, row_size, PIECES)), dma((slots, PIECES)), dma((PIECES,)), dma((PIECES,)),
                dma((slots, PIECES)), dma((slots, PIECES)), dma((row_size,)), dma((slots,)), dma((slots,)), dma((slots,)),
            ],
            compiler_params=pltpu.CompilerParams(
                collective_id=0, has_side_effects=True, vmem_limit_bytes=60 * 2**20
            ),
            name='purify',
        )(ham_blk, spec_bounds.T, occ_count)
        return density, energy[:, 0, 0]

    mat_spec = P('spin', 'row', 'col')
    return jax.shard_map(local_purify, mesh=mesh, in_specs=(mat_spec, P('spin', None), P('spin')), out_specs=(mat_spec, P('spin')), check_vma=False)
```
